32 devices in a mesh: ma: 16 (over z, x, core), af: 2 (over y).
Axes of the slice: x: 2, y: 2, z: 4, core: 2. Of those that a mesh axis runs over, the one named last changes fastest.
Arguments:
- coeffs: bfloat16 [512, 128, 2049], P('ma', 'af'), parts along dimension 1, may hold values from -6 to 6
- legendre: bfloat16 [512, 256, 2049], P('ma'), may hold values from -0.1875 to 0.1875
- assign: int32 [512], P('ma'), may hold values from 0 to 511, each once
Outputs:
- fourier: float32 [512, 128, 1024], P('ma', 'af'), parts along dimension 1
The draws below stay inside these ranges and needn't reach their ends.
There are 2 independent parts, one for each index of `af`. The reference program is written for one: setup_inputs(seed, part) draws one part's arguments, and reference() takes and returns one part's arrays. A program takes and returns all parts, laid end to end along the dimension named above; an argument that names none is the same for every part. Nothing has to cross between parts.
Inputs may be any that keep to these rules, and one draw needn't show every extreme that they name: Slot s carries the wavenumbers assign[s] and 2047 - assign[s]; every pair appears once.
All inputs are finite; a program needn't handle non-finite values.
Results may differ from the reference program's by a relative error of at most 0.0003.
Values sent between devices are 32-bit elements; how exact they have to be, the bound alone decides.
A program may use at most 128 MiB of HBM per device.

```python
import jax
import jax.numpy as jnp
from jax import lax

TRUNC = 2047
PAIRS = 512
HLAT = 256
FIELDS = 32
KP = 2049
COLS = 64


def block_scale(key, extent, pieces, low, high):
    level, own = 1.0, jax.random.fold_in(key, 6)
    for dim, blocks in pieces:
        heights = jnp.exp(jax.random.uniform(jax.random.fold_in(own, dim), (blocks,), jnp.float32, low / len(pieces), high / len(pieces)))
        level = level * jnp.repeat(heights, extent[dim] // blocks).reshape([-1 if axis == dim else 1 for axis in range(len(extent))])
    return level


def centred(rng, shape, scale, most, shards=(), held_as=jnp.bfloat16):
    gain = block_scale(rng, shape, shards, -0.22, 0.18) if shards else 1.0
    entries = jax.random.normal(rng, shape, jnp.float32) * scale * gain
    return jnp.minimum(jnp.maximum(entries, -most), most).astype(held_as)


def setup_inputs(seed: int = 0, part: int = 0) -> dict:
    seeds = jax.random.split(jax.random.key(seed), 4)
    part_keys = jax.random.split(jax.random.fold_in(seeds[3], part), 4)
    coeffs = centred(part_keys[0], (PAIRS, COLS, KP), 1.0, 6.0, ((0, 16),))
    legendre = centred(seeds[1], (PAIRS, HLAT, KP), (KP // 2) ** -0.5, 0.1875, ((0, 16),))
    assign = jax.random.permutation(seeds[2], PAIRS).astype(jnp.int32)
    return {"coeffs": coeffs, "legendre": legendre, "assign": assign}


def slot_values(legendre_rows, coeff_rows, pair):
    entry = jnp.arange(KP, dtype=jnp.int32)
    first_len = (TRUNC + 1 - pair).astype(jnp.int32)
    second = entry >= first_len
    degree_gap = jnp.where(second, entry - first_len, entry)
    odd_gap = (degree_gap % 2) == 1
    group_masks = jnp.stack([
        jnp.logical_and(jnp.logical_not(second), jnp.logical_not(odd_gap)),
        jnp.logical_and(jnp.logical_not(second), odd_gap),
        jnp.logical_and(second, jnp.logical_not(odd_gap)),
        jnp.logical_and(second, odd_gap)], axis=0).astype(jnp.float32)
    masked = coeff_rows.astype(jnp.float32)[None, :, :] * group_masks[:, None, :]
    partial_value = jnp.einsum('hk,gck->hcg', legendre_rows.astype(jnp.float32), masked)
    north_rows = partial_value[:, :, 0::2] + partial_value[:, :, 1::2]
    south_rows = partial_value[:, :, 0::2] - partial_value[:, :, 1::2]
    return jnp.concatenate([north_rows, south_rows[::-1]], axis=0)


def reference(coeffs, legendre, assign):
    def one_slot(items):
        return slot_values(items[0], items[1], items[2])

    values = lax.map(one_slot, (legendre, coeffs, assign))
    values = jnp.transpose(values, (1, 2, 0, 3)).reshape(2 * HLAT, 2 * FIELDS, 2 * PAIRS)
    column = jnp.arange(2 * PAIRS, dtype=jnp.int32)
    owner_pair = assign[column // 2]
    column_place = jnp.where(column % 2 == 0, owner_pair, 2 * PAIRS - 1 - owner_pair).astype(jnp.int32)
    fourier = jnp.zeros((2 * HLAT, 2 * FIELDS, 2 * PAIRS), jnp.float32)
    return fourier.at[:, :, column_place].set(values)
```

```python
import functools

import jax
import jax.numpy as jnp
from jax import lax
from jax.experimental import pallas as pl
from jax.experimental.pallas import tpu as pltpu
from jax.sharding import PartitionSpec as P

TRUNC = 2047
ROWS_PER_STEP = 4
PIECES = 4
FIRST_PIECES = 1
LAST_PIECES = 1


def group_kernel(pairs_ref, coeff_ref, out_ref, *, start):
    held, columns, width = coeff_ref.shape
    pack = 16
    for slot in range(held):
        pair = pairs_ref[start + pl.program_id(0) * held + slot]
        group_slot(TRUNC + 1 - pair, coeff_ref.at[slot], out_ref.at[slot], pack)


def group_slot(first_len, coeff_ref, out_ref, pack):
    columns, width = coeff_ref.shape
    entry = lax.broadcasted_iota(jnp.int32, (pack, width), 1)
    first = entry < first_len
    odd_gap = (jnp.where(first, entry, entry - first_len) & 1) == 1
    sign = jnp.where(odd_gap, -1.0, 1.0)
    scales = [
        jnp.where(first, 1.0, 0.0),
        jnp.where(first, 0.0, 1.0),
        jnp.where(first, sign, 0.0),
        jnp.where(first, 0.0, sign),
    ]
    scales = [scale.astype(out_ref.dtype) for scale in scales]
    for low in range(0, columns, pack):
        values = coeff_ref[low:low + pack, :]
        for index, scale in enumerate(scales):
            at = index * columns + low
            out_ref[at:at + pack, :] = values * scale


def group_rows(coeffs, assign, start, part):
    _, columns, width = coeffs.shape
    held = 2 if part % 2 == 0 and start % 2 == 0 else 1
    return pl.pallas_call(
        functools.partial(group_kernel, start=start),
        grid_spec=pltpu.PrefetchScalarGridSpec(
            num_scalar_prefetch=1,
            grid=(part // held,),
            in_specs=[pl.BlockSpec((held, columns, width), lambda i, p: (start // held + i, 0, 0))],
            out_specs=pl.BlockSpec((held, 4 * columns, width), lambda i, p: (i, 0, 0)),
        ),
        out_shape=jax.ShapeDtypeStruct((part, 4 * columns, width), coeffs.dtype),
        cost_estimate=pl.CostEstimate(flops=0, transcendentals=0, bytes_accessed=part * columns * width * 10),
        name="group_rows",
    )(assign, coeffs)


def band_kernel(own_ref, *refs, band):
    out_ref = refs[-1]
    bands = out_ref.shape[0]
    south = pl.program_id(0)
    at = 0
    for value_ref in refs[:-1]:
        for slot in range(value_ref.shape[0]):
            rows = value_ref[slot].T
            for index in range(bands):
                to = jnp.where(south == 1, bands - 1 - index, index)
                out_ref[to, :band, at, :] = rows[index * band:(index + 1) * band]
            at += 1
    if out_ref.shape[1] > band:
        own = jnp.broadcast_to(own_ref[...], (bands, 1, at, own_ref.shape[-1]))
        out_ref[:, band:] = own


def band_rows(values, own, devices, extra):
    _, lanes, lat_half = values[0].shape
    part = sum(value.shape[0] for value in values)
    lanes //= 2
    bands = devices // 2
    band = lat_half // bands
    return pl.pallas_call(
        functools.partial(band_kernel, band=band),
        grid=(2,),
        in_specs=[pl.BlockSpec((1, lanes), lambda i: (0, 0))]
        + [pl.BlockSpec((value.shape[0], lanes, lat_half), lambda i: (0, i, 0)) for value in values],
        out_specs=pl.BlockSpec((bands, band + extra, part, lanes), lambda i: (i, 0, 0, 0)),
        out_shape=jax.ShapeDtypeStruct((devices, band + extra, part, lanes), jnp.float32),
        cost_estimate=pl.CostEstimate(
            flops=0, transcendentals=0, bytes_accessed=part * lanes * lat_half * 16
        ),
        name="band_rows",
    )(own, *values)


def chunk_rows(coeffs, legendre, assign, own, pieces, devices, extra):
    values = []
    for start, part in pieces:
        groups = group_rows(coeffs, assign, start, part)
        functions = lax.optimization_barrier(legendre[start:start + part])
        value = jnp.einsum("sgk,shk->sgh", groups, functions, preferred_element_type=jnp.float32)
        value, coeffs, legendre = lax.optimization_barrier((value, coeffs, legendre))
        values.append(value)
    return band_rows(values, own, devices, extra)


def place_kernel(flip_ref, pairs_ref, *refs, held):
    out_ref, place = refs[-2:]
    value_refs = refs[:-3] if held else refs[:-2]
    devices, rows, _, lanes = value_refs[0].shape
    count, total = place.shape
    total //= 2
    columns = lanes // 2

    @pl.when(pl.program_id(0) == 0)
    def _():
        pairs = jnp.broadcast_to(pairs_ref[...], (count, total))
        lane = lax.broadcasted_iota(jnp.int32, (count, total), 1)
        place[:, :total] = (pairs == lane).astype(jnp.bfloat16)
        place[:, total:] = (total - 1 - pairs == lane).astype(jnp.bfloat16)

    def by_lane(row):
        tiles = [ref[:, row].reshape(devices * ref.shape[2], lanes).T for ref in value_refs]
        return tiles[0] if len(tiles) == 1 else jnp.concatenate(tiles, axis=1)

    flip = flip_ref[0]
    values = jnp.concatenate([by_lane(row)[None] for row in range(rows)], axis=0)
    for half in range(2):
        mine = values[:, half * columns:(half + 1) * columns].reshape(rows * columns, count)
        high = mine.astype(jnp.bfloat16)
        low = (mine - high.astype(jnp.float32)).astype(jnp.bfloat16)
        span = slice(half * total, (half + 1) * total)
        placed = jnp.dot(high, place[:, span], preferred_element_type=jnp.float32)
        placed += jnp.dot(low, place[:, span], preferred_element_type=jnp.float32)
        placed = placed.reshape(rows, columns, total)
        for row in range(rows):
            to = jnp.where(flip == 1, rows - 1 - row, row)
            block = placed[row]
            if held:
                block += refs[-3][to, :, span]
            out_ref[to, :, span] = block


def place_columns(received, pairs, flip, band, total, placed):
    devices, _, _, lanes = received[0].shape
    count = pairs.shape[0]
    held = placed is not None
    steps = band // ROWS_PER_STEP
    columns = lanes // 2
    out_spec = pl.BlockSpec(
        (ROWS_PER_STEP, columns, 2 * total),
        lambda i, f: (jnp.where(f[0] == 1, steps - 1 - i, i), 0, 0),
    )
    return pl.pallas_call(
        functools.partial(place_kernel, held=held),
        grid_spec=pltpu.PrefetchScalarGridSpec(
            num_scalar_prefetch=1,
            grid=(steps,),
            in_specs=[pl.BlockSpec((count, 1), lambda i, f: (0, 0))]
            + [
                pl.BlockSpec((devices, ROWS_PER_STEP, block.shape[2], lanes), lambda i, f: (0, i, 0, 0))
                for block in received
            ]
            + ([out_spec] if held else []),
            out_specs=out_spec,
            scratch_shapes=[pltpu.VMEM((count, 2 * total), jnp.bfloat16)],
        ),
        out_shape=jax.ShapeDtypeStruct((band, columns, 2 * total), jnp.float32),
        cost_estimate=pl.CostEstimate(
            flops=4 * band * columns * count * total, transcendentals=0, bytes_accessed=32 * band * columns * total
        ),
        name="place_columns",
    )(flip, pairs, *received, *([placed] if held else []))


def shards(coeffs, legendre, assign):
    devices = lax.axis_size("ma")
    slots, columns, _ = coeffs.shape
    band = 2 * legendre.shape[1] // devices
    piece = max(slots // PIECES, 1)
    starts = list(range(0, slots, piece))
    bounds = [0, FIRST_PIECES, len(starts) - LAST_PIECES, len(starts)]
    own = jnp.pad(assign.astype(jnp.float32), (0, 2 * columns - slots))[None, :]
    flip = (lax.axis_index("ma") >= devices // 2).astype(jnp.int32)[None]
    received = []
    parts = []
    for low, high in zip(bounds, bounds[1:]):
        extra = 1 if low == 0 else 0
        pieces = [(start, min(piece, slots - start)) for start in starts[low:high]]
        rows = chunk_rows(coeffs, legendre, assign, own, pieces, devices, extra)
        rows, coeffs, legendre = lax.optimization_barrier((rows, coeffs, legendre))
        received.append(lax.all_to_all(rows, "ma", 0, 0, tiled=True))
        parts.append(sum(part for _, part in pieces))
    all_pairs = received[0][:, band, 0, :slots].astype(jnp.int32)
    ends = [sum(parts[:n]) for n in range(len(parts) + 1)]
    pairs = [all_pairs[:, low:high].reshape(-1, 1) for low, high in zip(ends, ends[1:])]
    early = jnp.concatenate(pairs[:-1], axis=0)
    placed = place_columns(received[:-1], early, flip, band, devices * slots, None)
    return place_columns(received[-1:], pairs[-1], flip, band, devices * slots, placed)


def solution(mesh):
    return jax.shard_map(
        shards,
        mesh=mesh,
        in_specs=(P("ma", "af", None), P("ma", None, None), P("ma")),
        out_specs=P("ma", "af", None),
        check_vma=False,
    )
```
